32 devices in a mesh: member: 8 (over y, x, core), lat: 4 (over z).
Axes of the slice: x: 2, y: 2, z: 4, core: 2. Of those that a mesh axis runs over, the one named last changes fastest.
Arguments:
- ensemble: float32 [16, 3, 1, 32, 1440], P('member', None, None, 'lat'), may hold values from -6 to 6
- observation: float32 [3, 1, 32, 1440], P(None, None, 'lat'), may hold values from -6 to 6
- valid_mask: int32 [16], P('member'), may hold values from 0 to 1, as said below
- band_start: int32 [4], P('lat'), may hold values from 0 to 713
Outputs:
- crps_field: float32 [3, 1, 32, 1440], P(None, None, ('lat', 'member'))
- score_table: float32 [3, 1], replicated
The draws below stay inside these ranges and needn't reach their ends.
Inputs may be any that keep to these rules, and one draw needn't show every extreme that they name: `valid_mask`: exactly 13 entries are 1, at positions drawn afresh.
All inputs are finite; a program needn't handle non-finite values.
Results may differ from the reference program's by a relative error of at most 0.0001.
Values sent between devices are 32-bit elements; how exact they have to be, the bound alone decides.
A program may use at most 64 MiB of HBM per device.

```python
import math
import jax
import jax.numpy as jnp
from jax import lax

GRID_LAT = 721
GRID_LON = 1440
VARS = 3
LEADS = 1
LAT_DEV = 8
MEMBERS = 16
VALID = 13
LAT = 32
N_LAT = 4


def draw_valid_mask(key, part):
    shuffled = jax.random.permutation(jax.random.fold_in(key, 17), MEMBERS)
    return (shuffled < VALID).astype(jnp.int32)


def touch_ends(drawn, key, low, top_value):
    dims = drawn.shape
    spot = [jax.random.randint(jax.random.fold_in(key, axis), (), 0, dims[axis]) for axis in range(len(dims))]
    drawn = drawn.at[tuple(spot)].set(low)
    longest = dims.index(max(dims))
    spot[longest] = (spot[longest] + 1) % dims[longest]
    return drawn.at[tuple(spot)].set(top_value)


def steps_of(stream_key, shape, pieces, low, high):
    gain = 1.0
    for dim, shards_of in pieces:
        steps = jax.random.uniform(jax.random.fold_in(jax.random.fold_in(stream_key, 6), dim), (shards_of,), jnp.float32, low / len(pieces), high / len(pieces))
        gain = gain * jnp.repeat(jnp.exp(steps), shape[dim] // shards_of).reshape((-1,) + (1,) * (len(shape) - 1 - dim))
    return gain


def scatter_about(own_key, extent, scale, bound, split=(), kind=jnp.bfloat16):
    values = scale * jax.random.normal(own_key, extent, jnp.float32)
    if split:
        values = values * steps_of(own_key, extent, split, -0.22, 0.18)
    return jnp.clip(values, -bound, bound).astype(kind)


def setup_inputs(seed: int = 0) -> dict:
    arg_keys = jax.random.split(jax.random.key(seed), 5)
    return {
        "ensemble": scatter_about(arg_keys[0], (MEMBERS, VARS, LEADS, LAT, GRID_LON), 1.0, 6.0, ((0, 8), (3, 4)), jnp.float32),
        "observation": scatter_about(arg_keys[1], (VARS, LEADS, LAT, GRID_LON), 1.0, 6.0, ((2, 4),), jnp.float32),
        "valid_mask": draw_valid_mask(jax.random.fold_in(arg_keys[4], 71), 0),
        "band_start": touch_ends(jax.random.randint(arg_keys[3], (N_LAT,), 0, GRID_LAT - LAT_DEV + 1), jax.random.fold_in(arg_keys[3], 1), 0, GRID_LAT - LAT_DEV).astype(jnp.int32),
    }


def reference(ensemble, observation, valid_mask, band_start):
    member_flags = valid_mask.astype(jnp.float32)
    valid_count = jnp.sum(member_flags)
    flag_column = member_flags[:, None, None, None, None]
    skill_term = jnp.sum(flag_column * jnp.abs(ensemble - observation[None]), axis=0)

    def accumulate(running_sum, block_item):
        member_slab, member_flag = block_item
        distance = jnp.sum(flag_column * jnp.abs(member_slab[None] - ensemble), axis=0)
        return running_sum + member_flag * distance, None

    spread, unused = lax.scan(accumulate, jnp.zeros(observation.shape, jnp.float32), (ensemble, member_flags))
    crps_field = skill_term / valid_count - spread / (2.0 * valid_count * (valid_count - 1.0))
    row_index = (band_start[:, None] + jnp.arange(LAT_DEV, dtype=jnp.int32)[None, :]).reshape(-1).astype(jnp.float32)
    weight = jnp.cos((90.0 - row_index * 180.0 / (GRID_LAT - 1)) * math.pi / 180.0)
    score_table = jnp.sum(crps_field * weight[:, None], axis=(2, 3)) / (N_LAT * LAT_DEV * GRID_LON)
    return (crps_field, score_table)
```

```python
import functools
import math

import jax
import jax.numpy as jnp
from jax import lax
from jax.experimental import pallas as pl
from jax.experimental.pallas import tpu as pltpu
from jax.sharding import PartitionSpec as P

GRID_LAT = 721
GRID_LON = 1440
LANES = 128
SUBLANES = 8
FILL = 1e30
VMEM_BYTES = 67_043_328 - 65_536
MESH = pl.DeviceIdType.MESH


def round_up(value, step):
    return (value + step - 1) // step * step


def sort_pairs(count):
    pairs = []
    p = 1
    while p < count:
        k = p
        while k >= 1:
            for j in range(k % p, count - k, 2 * k):
                for i in range(min(k, count - j - k)):
                    if (i + j) // (2 * p) == (i + j + k) // (2 * p):
                        pairs.append((i + j, i + j + k))
            k //= 2
        p *= 2
    return pairs


def other(me, k, n):
    partner, bit = 0, 1
    while bit < n:
        here = (me // bit) % 2
        partner = partner + bit * (1 - here if k & bit else here)
        bit *= 2
    return partner


class Packing:
    def __init__(self, units, lon):
        self.units, self.full, self.tail = units, lon // LANES, lon % LANES
        self.beside = LANES // self.tail if self.tail else 1
        self.tails = round_up(units, self.beside) // self.beside if self.tail else 0
        self.lines = units * self.full + self.tails
        self.used = (units - 1) % self.beside * self.tail + self.tail

    def line(self, load, number):
        if number < self.units * self.full:
            return load(number // self.full, number % self.full * LANES, LANES)
        first = (number - self.units * self.full) * self.beside
        last = min(first + self.beside, self.units)
        parts = [load(u, self.full * LANES, self.tail) for u in range(first, last)]
        empty = LANES - self.tail * len(parts)
        if empty:
            parts.append(jnp.zeros((SUBLANES, empty), jnp.float32))
        return jnp.concatenate(parts, axis=1) if len(parts) > 1 else parts[0]

    def mask(self, unit, line, lane):
        inside = (line >= unit * self.full) & (line < (unit + 1) * self.full)
        if self.tail:
            low = unit % self.beside * self.tail
            at = self.units * self.full + unit // self.beside
            inside |= (line == at) & (lane >= low) & (lane < low + self.tail)
        return inside

    def pieces(self):
        for u in range(self.units):
            for c in range(self.full):
                yield u, c * LANES, LANES, u * self.full + c, 0
            if self.tail:
                at = self.units * self.full + u // self.beside
                yield u, self.full * LANES, self.tail, at, u % self.beside * self.tail


def kernel(
    n, nz, ens_ref, obs_ref, mask_ref, band_ref, field_ref, table_ref,
    ens_v, obs_v, mask_s, packet, obs_rows, gathered, partials,
    load_sem, send_sem, recv_sem, psend_sem, precv_sem, ready_sem,
):
    held, variables, leads, rows, lon = ens_ref.shape
    units = variables * leads
    packing = Packing(units, lon)
    lines = packing.lines
    pitch = packet.shape[0] // n
    stride = obs_rows.shape[0] // n
    slots = n * held
    total = n * nz
    me = lax.axis_index("member")
    band = lax.axis_index("lat")
    mine = band * n + me

    loads = [pltpu.make_async_copy(mask_ref, mask_s, load_sem.at[held + 1])]
    loads += [pltpu.make_async_copy(ens_ref.at[m], ens_v.at[m], load_sem.at[m]) for m in range(held)]
    loads.append(pltpu.make_async_copy(obs_ref, obs_v, load_sem.at[held]))
    plane = [{"member": other(me, k, n), "lat": band} for k in range(1, n)]
    line_peers = [{"member": me, "lat": lax.rem(band + k, nz)} for k in range(1, nz)]
    barrier = pltpu.get_barrier_semaphore()
    for peer in plane[::-1] + line_peers:
        pl.semaphore_signal(barrier, inc=1, device_id=peer, device_id_type=MESH)
    for load in loads:
        load.start()

    loads[0].wait()
    free = lax.broadcasted_iota(jnp.int32, (SUBLANES, LANES), 1) >= packing.used
    for m in range(held):
        loads[1 + m].wait()
        flag = jnp.full((SUBLANES, LANES), mask_s[m], jnp.int32)
        keep = flag != 0
        for block in range(0, rows, SUBLANES):
            base = block * pitch

            def load(u, low, wide):
                return ens_v[m, u // leads, u % leads, pl.ds(block, SUBLANES), pl.ds(low, wide)]

            for line in range(lines):
                value = jnp.where(keep, packing.line(load, line), FILL)
                if line == lines - 1:
                    value = jnp.where(free, flag.astype(jnp.float32), value)
                packet[pl.ds(base + m * lines + line, SUBLANES, stride=pitch), :] = value
            for line in range(held * lines + m, pitch, held):
                packet[pl.ds(base + line, SUBLANES, stride=pitch), :] = jnp.zeros_like(value)

    pl.semaphore_wait(barrier, n - 1 + nz - 1)

    sends = []
    for k in sorted(range(1, n), key=lambda k: (-bin(k // 2).count("1"), k)):
        sends.append(
            pltpu.make_async_remote_copy(
                src_ref=packet.at[
                    pl.ds(pl.multiple_of(plane[k - 1]["member"] * pitch, SUBLANES), held * lines)
                ],
                dst_ref=gathered.at[
                    pl.ds(pl.multiple_of(me * pitch, SUBLANES), held * lines)
                ],
                send_sem=send_sem.at[k],
                recv_sem=recv_sem.at[k],
                device_id=plane[k - 1],
                device_id_type=MESH,
            )
        )
        sends[-1].start()
    for peer in line_peers:
        pl.semaphore_signal(ready_sem, inc=1, device_id=peer, device_id_type=MESH)

    loads[1 + held].wait()
    for block in range(0, rows, SUBLANES):

        def load(u, low, wide):
            return obs_v[u // leads, u % leads, pl.ds(block, SUBLANES), pl.ds(low, wide)]

        for line in range(lines):
            obs_rows[pl.ds(block * stride + line, SUBLANES, stride=stride), :] = packing.line(
                load, line
            )
    gathered[pl.ds(pl.multiple_of(me * pitch, SUBLANES), pitch), :] = packet[
        pl.ds(pl.multiple_of(me * pitch, SUBLANES), pitch), :
    ]
    row_number = jnp.full((1, LANES), band_ref[0] + me, jnp.int32).astype(jnp.float32)
    weight = jnp.cos((90.0 - row_number * 180.0 / (GRID_LAT - 1)) * math.pi / 180.0)
    pl.semaphore_wait(ready_sem, nz - 1)

    for send in sends:
        send.wait_recv()

    flags = jnp.concatenate(
        [
            gathered[pl.ds(s // held * pitch + s % held * lines + lines - 1, 1), :]
            for s in range(slots)
        ],
        axis=0,
    )
    count = jnp.sum(flags, axis=0, keepdims=True)
    count = jnp.where(free[:1], count, 0.0)
    count = jnp.max(count, axis=1, keepdims=True)
    count = jnp.broadcast_to(count, (SUBLANES, LANES))
    per_one = 1.0 / count
    per_pair = per_one / (count - 1.0)
    skill_weight, spread_weight = [], []
    for i in range(slots):
        counted = i < count
        skill_weight.append(jnp.where(counted, per_one, 0.0))
        spread_weight.append(jnp.where(counted, (2.0 * i + 1.0 - count) * per_pair, 0.0))

    network = sort_pairs(slots)
    sums = [None] * units
    blocks = []
    lane = lax.broadcasted_iota(jnp.int32, (SUBLANES, LANES), 1)
    for j in range(0, lines, SUBLANES):
        x = [
            gathered[pl.ds(s // held * pitch + s % held * lines + j, SUBLANES), :]
            for s in range(slots)
        ]
        for a, b in network:
            x[a], x[b] = jnp.minimum(x[a], x[b]), jnp.maximum(x[a], x[b])
        truth = obs_rows[pl.ds(pl.multiple_of(me * stride + j, SUBLANES), SUBLANES), :]
        score = None
        for i in range(slots):
            term = skill_weight[i] * jnp.abs(x[i] - truth) - spread_weight[i] * x[i]
            score = term if score is None else score + term
        blocks.append(score)
        line = j + lax.broadcasted_iota(jnp.int32, (SUBLANES, LANES), 0)
        for u in range(units):
            part = jnp.where(packing.mask(u, line, lane), score, 0.0)
            sums[u] = part if sums[u] is None else sums[u] + part

    lane = lax.broadcasted_iota(jnp.int32, (1, LANES), 1)
    row = jnp.zeros((1, LANES), jnp.float32)
    for u in range(units):
        one = jnp.sum(jnp.sum(sums[u], axis=0, keepdims=True), axis=1, keepdims=True)
        row = jnp.where(lane == u, one, row)
    partials[pl.ds(mine, 1), :] = row * weight

    def share_with(far):
        return pltpu.make_async_remote_copy(
            src_ref=partials.at[pl.ds(mine, 1)],
            dst_ref=partials.at[pl.ds(mine, 1)],
            send_sem=psend_sem.at[0],
            recv_sem=precv_sem.at[0],
            device_id={"member": far % n, "lat": far // n},
            device_id_type=MESH,
        )

    def share_from(far):
        return pltpu.make_async_remote_copy(
            src_ref=partials.at[pl.ds(mine, 1)],
            dst_ref=partials.at[pl.ds(far, 1)],
            send_sem=psend_sem.at[0],
            recv_sem=precv_sem.at[0],
            device_id={"member": far % n, "lat": far // n},
            device_id_type=MESH,
        )

    for far in range(total):
        pl.when(far != mine)(lambda far=far: share_with(far).start())

    for u, low, wide, at, first in packing.pieces():
        piece = blocks[at // SUBLANES][at % SUBLANES : at % SUBLANES + 1, first : first + wide]
        field_ref[u // leads, u % leads, :, pl.ds(low, wide)] = piece

    for send in sends:
        send.wait_send()
    everything = pltpu.make_async_copy(partials.at[pl.ds(1, total - 1)], partials.at[pl.ds(1, total - 1)], psend_sem.at[0])
    everything.wait()
    everything = pltpu.make_async_copy(partials.at[pl.ds(1, total - 1)], partials.at[pl.ds(1, total - 1)], precv_sem.at[0])
    everything.wait()
    summed = jnp.sum(partials[...], axis=0, keepdims=True)
    table_ref[...] = summed[:, :units] / (nz * rows * GRID_LON)


def write_out(field_ref, table_ref, field_out, table_out, sem):
    copies = [
        pltpu.make_async_copy(field_ref, field_out, sem.at[0]),
        pltpu.make_async_copy(table_ref, table_out, sem.at[1]),
    ]
    for copy in copies:
        copy.start()
    for copy in copies:
        copy.wait()


def on_device(n, nz, ensemble, observation, valid_mask, band_start):
    held, variables, leads, rows, lon = ensemble.shape
    assert rows == n and rows % SUBLANES == 0
    units = variables * leads
    packing = Packing(units, lon)
    assert packing.tails and packing.used < LANES
    pitch = round_up(held * packing.lines, SUBLANES)
    stride = round_up(packing.lines, SUBLANES)
    total = n * nz
    field, table = pl.pallas_call(
        functools.partial(kernel, n, nz),
        out_shape=(
            pltpu.VMEM((variables, leads, rows // n, lon), jnp.float32),
            pltpu.VMEM((1, units), jnp.float32),
        ),
        in_specs=[pl.BlockSpec(memory_space=pltpu.HBM)] * 3 + [pl.BlockSpec(memory_space=pltpu.SMEM)],
        out_specs=(
            pl.BlockSpec(memory_space=pltpu.VMEM),
            pl.BlockSpec(memory_space=pltpu.VMEM),
        ),
        scratch_shapes=[
            pltpu.VMEM(ensemble.shape, jnp.float32),
            pltpu.VMEM(observation.shape, jnp.float32),
            pltpu.SMEM(valid_mask.shape, jnp.int32),
            pltpu.VMEM((n * pitch, LANES), jnp.float32),
            pltpu.VMEM((n * stride, LANES), jnp.float32),
            pltpu.VMEM((n * pitch + SUBLANES, LANES), jnp.float32),
            pltpu.VMEM((total, LANES), jnp.float32),
            pltpu.SemaphoreType.DMA((held + 2,)),
            pltpu.SemaphoreType.DMA((n,)),
            pltpu.SemaphoreType.DMA((n,)),
            pltpu.SemaphoreType.DMA((1,)),
            pltpu.SemaphoreType.DMA((1,)),
            pltpu.SemaphoreType.REGULAR,
        ],
        compiler_params=pltpu.CompilerParams(
            collective_id=0, has_side_effects=True, vmem_limit_bytes=VMEM_BYTES
        ),
        name="fair_crps",
    )(ensemble, observation, valid_mask, band_start)
    field, table = pl.pallas_call(
        write_out,
        out_shape=(
            jax.ShapeDtypeStruct(field.shape, jnp.float32),
            jax.ShapeDtypeStruct(table.shape, jnp.float32),
        ),
        in_specs=[pl.BlockSpec(memory_space=pltpu.VMEM)] * 2,
        out_specs=(pl.BlockSpec(memory_space=pltpu.HBM),) * 2,
        scratch_shapes=[pltpu.SemaphoreType.DMA((2,))],
        name="write_out",
    )(*(pltpu.with_memory_space_constraint(a, pltpu.VMEM) for a in (field, table)))
    return field, table.reshape(variables, leads)


def solution(mesh):
    placed = (
        P("member", None, None, "lat", None),
        P(None, None, "lat", None),
        P("member"),
        P("lat"),
    )
    return jax.shard_map(
        functools.partial(on_device, mesh.shape["member"], mesh.shape["lat"]),
        mesh=mesh,
        in_specs=placed,
        out_specs=(P(None, None, ("lat", "member"), None), P()),
        check_vma=False,
    )
```

```python
import functools
import math

import jax
import jax.numpy as jnp
from jax import lax
from jax.experimental import pallas as pl
from jax.experimental.pallas import tpu as pltpu
from jax.sharding import PartitionSpec as P

GRID_LAT = 721
LANES = 128
SUBLANES = 8
VMEM_BYTES = 67_043_328 - 65_536
MESH = pl.DeviceIdType.MESH


def round_up(value, step):
    return (value + step - 1) // step * step


def sort_pairs(count):
    pairs = []
    p = 1
    while p < count:
        k = p
        while k >= 1:
            for j in range(k % p, count - k, 2 * k):
                for i in range(min(k, count - j - k)):
                    if (i + j) // (2 * p) == (i + j + k) // (2 * p):
                        pairs.append((i + j, i + j + k))
            k //= 2
        p *= 2
    return pairs


def other(me, k, n):
    partner, bit = 0, 1
    while bit < n:
        here = (me // bit) % 2
        partner = partner + bit * (1 - here if k & bit else here)
        bit *= 2
    return partner


def steps(pair):
    return bin(pair).count("1")


class Packing:
    def __init__(self, units, lon):
        self.units, self.full, self.tail = units, lon // LANES, lon % LANES
        self.beside = LANES // self.tail if self.tail else 1
        self.tails = round_up(units, self.beside) // self.beside if self.tail else 0
        self.lines = units * self.full + self.tails
        self.used = (units - 1) % self.beside * self.tail + self.tail

    def line(self, load, number):
        if number >= self.tails:
            number -= self.tails
            return load(number // self.full, number % self.full * LANES, LANES)
        first = number * self.beside
        last = min(first + self.beside, self.units)
        parts = [load(u, self.full * LANES, self.tail) for u in range(first, last)]
        empty = LANES - self.tail * len(parts)
        if empty:
            parts.append(jnp.zeros((SUBLANES, empty), jnp.float32))
        return jnp.concatenate(parts, axis=1) if len(parts) > 1 else parts[0]

    def mask(self, unit, line, lane):
        start = self.tails + unit * self.full
        inside = (line >= start) & (line < start + self.full)
        if self.tail:
            low = unit % self.beside * self.tail
            inside |= (line == unit // self.beside) & (lane >= low) & (lane < low + self.tail)
        return inside

    def pieces(self):
        for u in range(self.units):
            for c in range(self.full):
                yield u, c * LANES, LANES, self.tails + u * self.full + c, 0
            if self.tail:
                yield u, self.full * LANES, self.tail, u // self.beside, u % self.beside * self.tail


class Layout:
    def __init__(self, held, lines):
        self.held, self.lines = held, lines
        self.split = max(lines // SUBLANES - 1, 1) * SUBLANES
        self.pitch = round_up(held * lines, SUBLANES)
        self.chunks = [(0, held * self.split), (held * self.split, held * (lines - self.split))]

    def row(self, m, line):
        if line < self.split:
            return m * self.split + line
        return self.held * self.split + m * (self.lines - self.split) + line - self.split


def kernel(
    n, nz, ens_ref, obs_ref, mask_ref, band_ref, field_ref, table_ref,
    ens_v, obs_v, mask_s, packet, obs_rows, gathered, partials,
    load_sem, send_sem, recv_sem, share_sem, wave_sem,
):
    held, variables, leads, rows, lon = ens_ref.shape
    units = variables * leads
    packing = Packing(units, lon)
    lines = packing.lines
    layout = Layout(held, lines)
    pitch, split = layout.pitch, layout.split
    stride = obs_rows.shape[0] // n
    slots = n * held
    total = n * nz
    me = lax.axis_index("member")
    band = lax.axis_index("lat")
    mine = band * n + me
    flag_line = packing.tails - 1

    plane = [{"member": other(me, k, n), "lat": band} for k in range(1, n)]
    above = {"member": me, "lat": lax.rem(band + 1, nz)}
    below = {"member": me, "lat": lax.rem(band + nz - 1, nz)}
    has_above = band < nz - 1
    has_below = band > 0

    def signal(sem, peer):
        pl.semaphore_signal(sem, inc=1, device_id=peer, device_id_type=MESH)

    barrier = pltpu.get_barrier_semaphore()
    for peer in plane[::-1]:
        signal(barrier, peer)
    mask_load = pltpu.make_async_copy(mask_ref, mask_s, load_sem.at[held + 1])
    ens_loads = [pltpu.make_async_copy(ens_ref.at[m], ens_v.at[m], load_sem.at[m]) for m in range(held)]
    obs_load = pltpu.make_async_copy(obs_ref, obs_v, load_sem.at[held])
    for load in [obs_load, mask_load] + ens_loads:
        load.start()
    pl.when(has_above)(lambda: signal(barrier, above))
    pl.when(has_below)(lambda: signal(barrier, below))

    mask_load.wait()
    obs_load.wait()
    free = lax.broadcasted_iota(jnp.int32, (SUBLANES, LANES), 1) >= packing.used

    def obs_line(block, line):
        def load(u, low, wide):
            return obs_v[u // leads, u % leads, pl.ds(block, SUBLANES), pl.ds(low, wide)]

        return packing.line(load, line)

    def pack(m, which):
        flag = jnp.full((SUBLANES, LANES), mask_s[m], jnp.int32)
        keep = flag != 0
        for block in range(0, rows, SUBLANES):

            def load(u, low, wide):
                return ens_v[m, u // leads, u % leads, pl.ds(block, SUBLANES), pl.ds(low, wide)]

            for line in which:
                value = jnp.where(keep, packing.line(load, line), obs_line(block, line))
                if line == flag_line:
                    value = jnp.where(free, flag.astype(jnp.float32), value)
                at = block * pitch + layout.row(m, line)
                packet[pl.ds(at, SUBLANES, stride=pitch), :] = value

    def send(chunk, to):
        low, size = layout.chunks[chunk]
        pltpu.make_async_remote_copy(
            src_ref=packet.at[pl.ds(to * pitch + low, size)],
            dst_ref=gathered.at[pl.ds(pl.multiple_of(me * pitch + low, SUBLANES), size)],
            send_sem=send_sem,
            recv_sem=recv_sem.at[chunk],
            device_id={"member": to, "lat": band},
            device_id_type=MESH,
        ).start()

    for m in range(held):
        ens_loads[m].wait()
        pack(m, range(lines))
    count_near = n - 1 + (band + nz - 1) // nz + (2 * nz - 2 - band) // nz
    pl.semaphore_wait(barrier, count_near)
    for to in sorted(range(n), key=lambda to: (-steps(to // 2), to)):

        @pl.when(to != me)
        def both(to=to):
            send(0, to)
            send(1, to)

    pl.when(band == nz - 1)(lambda: signal(wave_sem.at[1], below))
    for block in range(0, rows, SUBLANES):
        for line in range(lines):
            obs_rows[pl.ds(block * stride + line, SUBLANES, stride=stride), :] = obs_line(block, line)
    own = pl.ds(pl.multiple_of(me * pitch, SUBLANES), pitch)
    gathered[own, :] = packet[own, :]
    pl.when(has_below)(lambda: pl.semaphore_wait(wave_sem.at[0], 1))
    pl.when(has_above)(lambda: signal(wave_sem.at[0], above))
    row_number = jnp.full((1, LANES), band_ref[0] + me, jnp.int32).astype(jnp.float32)
    weight = jnp.cos((90.0 - row_number * 180.0 / (GRID_LAT - 1)) * math.pi / 180.0)
    pl.when(has_above)(lambda: pl.semaphore_wait(wave_sem.at[1], 1))
    pl.when(has_above & has_below)(lambda: signal(wave_sem.at[1], below))

    def arrived(sem, ref, size):
        whole = ref.at[pl.ds(0, size)]
        pltpu.make_async_copy(whole, whole, sem).wait()

    network = sort_pairs(slots)
    lane = lax.broadcasted_iota(jnp.int32, (SUBLANES, LANES), 1)
    below_line = lax.broadcasted_iota(jnp.int32, (SUBLANES, LANES), 0)
    sums = [None] * units
    per_skill = per_spread = None
    arrived(recv_sem.at[0], gathered, (n - 1) * layout.chunks[0][1])
    for j in range(0, lines, SUBLANES):
        if j == split:
            arrived(recv_sem.at[1], gathered, (n - 1) * layout.chunks[1][1])
        x = [
            gathered[pl.ds(s // held * pitch + layout.row(s % held, j), SUBLANES), :]
            for s in range(slots)
        ]
        if j == 0:
            flags = functools.reduce(jnp.add, x)
            flags = jnp.where((below_line == flag_line) & free, flags, 0.0)
            count = jnp.max(jnp.max(flags, axis=0, keepdims=True), axis=1, keepdims=True)
            count = jnp.broadcast_to(count, (SUBLANES, LANES))
            per_one = 1.0 / count
            per_spread = per_one / (count - 1.0)
            per_skill = per_one + (slots - count) * per_spread
        truth = obs_rows[pl.ds(pl.multiple_of(me * stride + j, SUBLANES), SUBLANES), :]
        skill = functools.reduce(jnp.add, [jnp.abs(value - truth) for value in x])
        for a, b in network:
            x[a], x[b] = jnp.minimum(x[a], x[b]), jnp.maximum(x[a], x[b])
        spread = functools.reduce(
            jnp.add,
            [(slots - 1.0 - 2.0 * i) * (x[slots - 1 - i] - x[i]) for i in range(slots // 2)],
        )
        score = per_skill * skill - per_spread * spread
        for u, low, wide, at, first in packing.pieces():
            if j <= at < j + SUBLANES:
                piece = score[at - j : at - j + 1, first : first + wide]
                field_ref[u // leads, u % leads, :, pl.ds(low, wide)] = piece
        for u in range(units):
            part = jnp.where(packing.mask(u, below_line + j, lane), score, 0.0)
            sums[u] = part if sums[u] is None else sums[u] + part

    lane = lax.broadcasted_iota(jnp.int32, (1, LANES), 1)
    row = jnp.zeros((1, LANES), jnp.float32)
    for u in range(units):
        one = jnp.sum(jnp.sum(sums[u], axis=0, keepdims=True), axis=1, keepdims=True)
        row = jnp.where(lane == u, one, row)
    partials[pl.ds(mine, 1), :] = row * weight

    def share_with(far):
        return pltpu.make_async_remote_copy(
            src_ref=partials.at[pl.ds(mine, 1)],
            dst_ref=partials.at[pl.ds(mine, 1)],
            send_sem=share_sem.at[0],
            recv_sem=share_sem.at[1],
            device_id={"member": far % n, "lat": far // n},
            device_id_type=MESH,
        )

    for far in range(total):
        pl.when(far != mine)(lambda far=far: share_with(far).start())
    arrived(send_sem, packet, (n - 1) * held * lines)
    arrived(share_sem.at[0], partials, total - 1)
    arrived(share_sem.at[1], partials, total - 1)
    summed = jnp.sum(partials[...], axis=0, keepdims=True)
    table_ref[...] = summed[:, :units] / (nz * rows * lon)


def write_out(field_ref, table_ref, field_out, table_out, sem):
    copies = [
        pltpu.make_async_copy(field_ref, field_out, sem.at[0]),
        pltpu.make_async_copy(table_ref, table_out, sem.at[1]),
    ]
    for copy in copies:
        copy.start()
    for copy in copies:
        copy.wait()


def on_device(n, nz, ensemble, observation, valid_mask, band_start):
    held, variables, leads, rows, lon = ensemble.shape
    assert rows == n and rows % SUBLANES == 0
    units = variables * leads
    packing = Packing(units, lon)
    assert packing.tails and packing.used < LANES
    assert n % 2 == 0 and packing.lines >= 2 * SUBLANES
    pitch = Layout(held, packing.lines).pitch
    stride = round_up(packing.lines, SUBLANES)
    total = n * nz
    field, table = pl.pallas_call(
        functools.partial(kernel, n, nz),
        out_shape=(
            pltpu.VMEM((variables, leads, rows // n, lon), jnp.float32),
            pltpu.VMEM((1, units), jnp.float32),
        ),
        in_specs=[pl.BlockSpec(memory_space=pltpu.HBM)] * 3 + [pl.BlockSpec(memory_space=pltpu.SMEM)],
        out_specs=(
            pl.BlockSpec(memory_space=pltpu.VMEM),
            pl.BlockSpec(memory_space=pltpu.VMEM),
        ),
        scratch_shapes=[
            pltpu.VMEM(ensemble.shape, jnp.float32),
            pltpu.VMEM(observation.shape, jnp.float32),
            pltpu.SMEM(valid_mask.shape, jnp.int32),
            pltpu.VMEM((n * pitch, LANES), jnp.float32),
            pltpu.VMEM((n * stride, LANES), jnp.float32),
            pltpu.VMEM((n * pitch + SUBLANES, LANES), jnp.float32),
            pltpu.VMEM((total, LANES), jnp.float32),
            pltpu.SemaphoreType.DMA((held + 2,)),
            pltpu.SemaphoreType.DMA,
            pltpu.SemaphoreType.DMA((2,)),
            pltpu.SemaphoreType.DMA((2,)),
            pltpu.SemaphoreType.REGULAR((2,)),
        ],
        compiler_params=pltpu.CompilerParams(
            collective_id=0, has_side_effects=True, vmem_limit_bytes=VMEM_BYTES
        ),
        name="fair_crps",
    )(ensemble, observation, valid_mask, band_start)
    field, table = pl.pallas_call(
        write_out,
        out_shape=(
            jax.ShapeDtypeStruct(field.shape, jnp.float32),
            jax.ShapeDtypeStruct(table.shape, jnp.float32),
        ),
        in_specs=[pl.BlockSpec(memory_space=pltpu.VMEM)] * 2,
        out_specs=(pl.BlockSpec(memory_space=pltpu.HBM),) * 2,
        scratch_shapes=[pltpu.SemaphoreType.DMA((2,))],
        name="write_out",
    )(*(pltpu.with_memory_space_constraint(a, pltpu.VMEM) for a in (field, table)))
    return field, table.reshape(variables, leads)


def solution(mesh):
    placed = (
        P("member", None, None, "lat", None),
        P(None, None, "lat", None),
        P("member"),
        P("lat"),
    )
    return jax.shard_map(
        functools.partial(on_device, mesh.shape["member"], mesh.shape["lat"]),
        mesh=mesh,
        in_specs=placed,
        out_specs=(P(None, None, ("lat", "member"), None), P()),
        check_vma=False,
    )
```

```python
import functools
import math

import jax
import jax.numpy as jnp
from jax import lax
from jax.experimental import pallas as pl
from jax.experimental.pallas import tpu as pltpu
from jax.sharding import PartitionSpec as P

GRID_LAT = 721
LANES = 128
SUBLANES = 8
VMEM_BYTES = 67_043_328 - 65_536
MESH = pl.DeviceIdType.MESH


def round_up(value, step):
    return (value + step - 1) // step * step


def sort_pairs(count):
    pairs = []
    p = 1
    while p < count:
        k = p
        while k >= 1:
            for j in range(k % p, count - k, 2 * k):
                for i in range(min(k, count - j - k)):
                    if (i + j) // (2 * p) == (i + j + k) // (2 * p):
                        pairs.append((i + j, i + j + k))
            k //= 2
        p *= 2
    return pairs


def steps(pair):
    return bin(pair).count("1")


class Packing:
    def __init__(self, units, lon):
        self.units, self.full, self.tail = units, lon // LANES, lon % LANES
        self.beside = LANES // self.tail if self.tail else 1
        self.tails = round_up(units, self.beside) // self.beside if self.tail else 0
        self.lines = units * self.full + self.tails
        self.used = (units - 1) % self.beside * self.tail + self.tail

    def line(self, load, number):
        if number >= self.tails:
            number -= self.tails
            return load(number // self.full, number % self.full * LANES, LANES)
        first = number * self.beside
        last = min(first + self.beside, self.units)
        parts = [load(u, self.full * LANES, self.tail) for u in range(first, last)]
        empty = LANES - self.tail * len(parts)
        if empty:
            parts.append(jnp.zeros((SUBLANES, empty), jnp.float32))
        return jnp.concatenate(parts, axis=1) if len(parts) > 1 else parts[0]

    def mask(self, unit, line, lane):
        start = self.tails + unit * self.full
        inside = (line >= start) & (line < start + self.full)
        if self.tail:
            low = unit % self.beside * self.tail
            inside |= (line == unit // self.beside) & (lane >= low) & (lane < low + self.tail)
        return inside

    def pieces(self):
        for u in range(self.units):
            for c in range(self.full):
                yield u, c * LANES, LANES, self.tails + u * self.full + c, 0
            if self.tail:
                yield u, self.full * LANES, self.tail, u // self.beside, u % self.beside * self.tail


class Layout:
    def __init__(self, held, lines):
        self.held, self.lines = held, lines
        self.split = max(lines // SUBLANES - 1, 1) * SUBLANES
        self.pitch = round_up(held * lines, SUBLANES)
        self.chunks = [(0, held * self.split), (held * self.split, held * (lines - self.split))]

    def row(self, m, line):
        if line < self.split:
            return m * self.split + line
        return self.held * self.split + m * (self.lines - self.split) + line - self.split


def kernel(
    n, nz, ens_ref, obs_ref, mask_ref, band_ref, field_ref, table_ref,
    ens_v, obs_v, mask_s, packet, obs_rows, gathered, partials,
    load_sem, send_sem, recv_sem, share_sem, round_sem, wave_sem,
):
    held, variables, leads, rows, lon = ens_ref.shape
    units = variables * leads
    packing = Packing(units, lon)
    lines = packing.lines
    layout = Layout(held, lines)
    pitch, split = layout.pitch, layout.split
    stride = obs_rows.shape[0] // n
    slots = n * held
    total = n * nz
    chips = n // 2
    depth = max(steps(pair) for pair in range(chips))
    bits = [1 << b for b in range(depth)]
    me = lax.axis_index("member")
    band = lax.axis_index("lat")
    mine = band * n + me
    flag_line = packing.tails - 1

    rest, change, held_bit = me, {}, {}
    for bit in [2 * bit for bit in bits[::-1]] + [1]:
        held_bit[bit] = rest >= bit
        change[bit] = jnp.where(held_bit[bit], -bit, bit)
        rest = jnp.where(held_bit[bit], rest - bit, rest)
    first_core = me - jnp.where(held_bit[1], 1, 0)

    def beside(pair, c):
        return first_core + sum(change[2 * bit] for bit in bits if pair & bit) + c

    partner = me + change[1]
    near = [beside(bit, c) for c in range(2) for bit in bits] + [partner]
    above = {"member": me, "lat": lax.rem(band + 1, nz)}
    below = {"member": me, "lat": lax.rem(band + nz - 1, nz)}
    has_above = band < nz - 1
    has_below = band > 0

    def signal(sem, peer):
        pl.semaphore_signal(sem, inc=1, device_id=peer, device_id_type=MESH)

    mask_load = pltpu.make_async_copy(mask_ref, mask_s, load_sem.at[held + 1])
    ens_loads = [pltpu.make_async_copy(ens_ref.at[m], ens_v.at[m], load_sem.at[m]) for m in range(held)]
    obs_load = pltpu.make_async_copy(obs_ref, obs_v, load_sem.at[held])
    for load in [obs_load, mask_load] + ens_loads:
        load.start()
    barrier = pltpu.get_barrier_semaphore()
    for to in near:
        signal(barrier, {"member": to, "lat": band})
    pl.when(has_above)(lambda: signal(barrier, above))
    pl.when(has_below)(lambda: signal(barrier, below))

    mask_load.wait()
    obs_load.wait()
    free = lax.broadcasted_iota(jnp.int32, (SUBLANES, LANES), 1) >= packing.used

    def obs_line(block, line):
        def load(u, low, wide):
            return obs_v[u // leads, u % leads, pl.ds(block, SUBLANES), pl.ds(low, wide)]

        return packing.line(load, line)

    def pack(m, which):
        flag = jnp.full((SUBLANES, LANES), mask_s[m], jnp.int32)
        keep = flag != 0
        for block in range(0, rows, SUBLANES):

            def load(u, low, wide):
                return ens_v[m, u // leads, u % leads, pl.ds(block, SUBLANES), pl.ds(low, wide)]

            for line in which:
                value = jnp.where(keep, packing.line(load, line), obs_line(block, line))
                if line == flag_line:
                    value = jnp.where(free, flag.astype(jnp.float32), value)
                at = block * pitch + layout.row(m, line)
                packet[pl.ds(at, SUBLANES, stride=pitch), :] = value

    def send(chunk, to):
        low, size = layout.chunks[chunk]
        pltpu.make_async_remote_copy(
            src_ref=packet.at[pl.ds(pl.multiple_of(to * pitch + low, SUBLANES), size)],
            dst_ref=gathered.at[pl.ds(pl.multiple_of(me * pitch + low, SUBLANES), size)],
            send_sem=send_sem,
            recv_sem=recv_sem.at[chunk],
            device_id={"member": to, "lat": band},
            device_id_type=MESH,
        ).start()

    def send_rows(pairs, cores, parts=(0, 1)):
        for c in cores:
            for pair in pairs:
                for part in parts:
                    send(part, beside(pair, c))

    across, along = bits[: (depth + 1) // 2], bits[(depth + 1) // 2 :]

    for m in range(held):
        ens_loads[m].wait()
        pack(m, range(lines))
    count_near = len(near) + (band + nz - 1) // nz + (2 * nz - 2 - band) // nz
    pl.semaphore_wait(barrier, count_near)
    def tell(far):
        for bit in bits:
            peer = me + change[2 * bit]
            low_kept = jnp.logical_not(held_bit[2]) if bit == 1 else held_bit[2] | (peer < 2)
            low_kept = low_kept | (peer < 2) if bit == 1 else low_kept
            go = functools.partial(signal, round_sem.at[far - 2], {"member": peer, "lat": band})
            if bit == bits[0]:
                pl.when(low_kept)(go)
            elif bit == bits[-1]:
                pl.when(jnp.logical_not(low_kept))(go)
            else:
                go()

    tell(2)
    for c in range(2):
        send_rows(across, [c], [0] if c else [0, 1])
        send_rows(along, [c])
    for far in range(2, depth + 1):
        if far > 2:
            tell(far)
        else:
            send(0, partner)
            send(1, partner)
        pl.semaphore_wait(round_sem.at[far - 2], depth - 1)
        send_rows([pair for pair in range(chips) if steps(pair) == far], range(2))
    send_rows(across, [1], [1])
    pl.when(band == nz - 1)(lambda: signal(wave_sem.at[1], below))
    for block in range(0, rows, SUBLANES):
        for line in range(lines):
            obs_rows[pl.ds(block * stride + line, SUBLANES, stride=stride), :] = obs_line(block, line)
    own = pl.ds(pl.multiple_of(me * pitch, SUBLANES), pitch)
    gathered[own, :] = packet[own, :]
    pl.when(has_below)(lambda: pl.semaphore_wait(wave_sem.at[0], 1))
    pl.when(has_above)(lambda: signal(wave_sem.at[0], above))
    row_number = jnp.full((1, LANES), band_ref[0] + me, jnp.int32).astype(jnp.float32)
    weight = jnp.cos((90.0 - row_number * 180.0 / (GRID_LAT - 1)) * math.pi / 180.0)
    pl.when(has_above)(lambda: pl.semaphore_wait(wave_sem.at[1], 1))
    pl.when(has_above & has_below)(lambda: signal(wave_sem.at[1], below))

    def arrived(sem, ref, size):
        whole = ref.at[pl.ds(0, size)]
        pltpu.make_async_copy(whole, whole, sem).wait()

    network = sort_pairs(slots)
    lane = lax.broadcasted_iota(jnp.int32, (SUBLANES, LANES), 1)
    below_line = lax.broadcasted_iota(jnp.int32, (SUBLANES, LANES), 0)
    sums = [None] * units
    raw = []
    arrived(recv_sem.at[0], gathered, (n - 1) * layout.chunks[0][1])
    for j in range(0, lines, SUBLANES):
        if j == split:
            arrived(recv_sem.at[1], gathered, (n - 1) * layout.chunks[1][1])
        x = [
            gathered[pl.ds(s // held * pitch + layout.row(s % held, j), SUBLANES), :]
            for s in range(slots)
        ]
        if j == 0:
            flags = functools.reduce(jnp.add, x)
            flags = jnp.where((below_line == flag_line) & free, flags, 0.0)
            count = jnp.max(jnp.max(flags, axis=0, keepdims=True), axis=1, keepdims=True)
            scale = 1.0 / (count * (count - 1.0))
        truth = obs_rows[pl.ds(pl.multiple_of(me * stride + j, SUBLANES), SUBLANES), :]
        skill = functools.reduce(jnp.add, [jnp.abs(value - truth) for value in x])
        for a, b in network:
            x[a], x[b] = jnp.minimum(x[a], x[b]), jnp.maximum(x[a], x[b])
        spread = functools.reduce(
            jnp.add,
            [(slots - 1.0 - 2.0 * i) * (x[slots - 1 - i] - x[i]) for i in range(slots // 2)],
        )
        score = (slots - 1.0) * skill - spread
        raw.append(score)
        for u in range(units):
            part = jnp.where(packing.mask(u, below_line + j, lane), score, 0.0)
            sums[u] = part if sums[u] is None else sums[u] + part

    lane = lax.broadcasted_iota(jnp.int32, (1, LANES), 1)
    row = jnp.zeros((1, LANES), jnp.float32)
    for u in range(units):
        one = jnp.sum(jnp.sum(sums[u], axis=0, keepdims=True), axis=1, keepdims=True)
        row = jnp.where(lane == u, one, row)
    partials[pl.ds(mine, 1), :] = row * (weight * scale)

    def share_with(far):
        return pltpu.make_async_remote_copy(
            src_ref=partials.at[pl.ds(mine, 1)],
            dst_ref=partials.at[pl.ds(mine, 1)],
            send_sem=send_sem,
            recv_sem=share_sem,
            device_id={"member": far % n, "lat": far // n},
            device_id_type=MESH,
        )

    for far in range(total):
        pl.when(far != mine)(lambda far=far: share_with(far).start())
    for u, low, wide, at, first in packing.pieces():
        piece = raw[at // SUBLANES][at % SUBLANES : at % SUBLANES + 1, first : first + wide]
        field_ref[u // leads, u % leads, :, pl.ds(low, wide)] = piece * scale
    arrived(send_sem, packet, (n - 1) * held * lines + total - 1)
    arrived(share_sem, partials, total - 1)
    summed = jnp.sum(partials[...], axis=0, keepdims=True)
    table_ref[...] = summed[:, :units] / (nz * rows * lon)


def write_out(field_ref, table_ref, field_out, table_out, sem):
    copies = [
        pltpu.make_async_copy(field_ref, field_out, sem.at[0]),
        pltpu.make_async_copy(table_ref, table_out, sem.at[1]),
    ]
    for copy in copies:
        copy.start()
    for copy in copies:
        copy.wait()


def on_device(n, nz, ensemble, observation, valid_mask, band_start):
    held, variables, leads, rows, lon = ensemble.shape
    assert rows == n and rows % SUBLANES == 0
    units = variables * leads
    packing = Packing(units, lon)
    assert packing.tails and packing.used < LANES
    assert n % 2 == 0 and packing.lines >= 2 * SUBLANES
    pitch = Layout(held, packing.lines).pitch
    depth = max(steps(pair) for pair in range(n // 2))
    assert depth > 1 and n == 2 ** (depth + 1)
    stride = round_up(packing.lines, SUBLANES)
    total = n * nz
    field, table = pl.pallas_call(
        functools.partial(kernel, n, nz),
        out_shape=(
            pltpu.VMEM((variables, leads, rows // n, lon), jnp.float32),
            pltpu.VMEM((1, units), jnp.float32),
        ),
        in_specs=[pl.BlockSpec(memory_space=pltpu.HBM)] * 3 + [pl.BlockSpec(memory_space=pltpu.SMEM)],
        out_specs=(
            pl.BlockSpec(memory_space=pltpu.VMEM),
            pl.BlockSpec(memory_space=pltpu.VMEM),
        ),
        scratch_shapes=[
            pltpu.VMEM(ensemble.shape, jnp.float32),
            pltpu.VMEM(observation.shape, jnp.float32),
            pltpu.SMEM(valid_mask.shape, jnp.int32),
            pltpu.VMEM((n * pitch, LANES), jnp.float32),
            pltpu.VMEM((n * stride, LANES), jnp.float32),
            pltpu.VMEM((n * pitch + SUBLANES, LANES), jnp.float32),
            pltpu.VMEM((total, LANES), jnp.float32),
            pltpu.SemaphoreType.DMA((held + 2,)),
            pltpu.SemaphoreType.DMA,
            pltpu.SemaphoreType.DMA((2,)),
            pltpu.SemaphoreType.DMA,
            pltpu.SemaphoreType.REGULAR((depth - 1,)),
            pltpu.SemaphoreType.REGULAR((2,)),
        ],
        compiler_params=pltpu.CompilerParams(
            collective_id=0, has_side_effects=True, vmem_limit_bytes=VMEM_BYTES
        ),
        name="fair_crps",
    )(ensemble, observation, valid_mask, band_start)
    field, table = pl.pallas_call(
        write_out,
        out_shape=(
            jax.ShapeDtypeStruct(field.shape, jnp.float32),
            jax.ShapeDtypeStruct(table.shape, jnp.float32),
        ),
        in_specs=[pl.BlockSpec(memory_space=pltpu.VMEM)] * 2,
        out_specs=(pl.BlockSpec(memory_space=pltpu.HBM),) * 2,
        scratch_shapes=[pltpu.SemaphoreType.DMA((2,))],
        name="write_out",
    )(*(pltpu.with_memory_space_constraint(a, pltpu.VMEM) for a in (field, table)))
    return field, table.reshape(variables, leads)


def solution(mesh):
    placed = (
        P("member", None, None, "lat", None),
        P(None, None, "lat", None),
        P("member"),
        P("lat"),
    )
    return jax.shard_map(
        functools.partial(on_device, mesh.shape["member"], mesh.shape["lat"]),
        mesh=mesh,
        in_specs=placed,
        out_specs=(P(None, None, ("lat", "member"), None), P()),
        check_vma=False,
    )
```

```python
import functools
import math

import jax
import jax.numpy as jnp
from jax import lax
from jax.experimental import pallas as pl
from jax.experimental.pallas import tpu as pltpu
from jax.sharding import PartitionSpec as P

GRID_LAT = 721
LANES = 128
SUBLANES = 8
VMEM_BYTES = 67_043_328 - 65_536
MESH = pl.DeviceIdType.MESH


def round_up(value, step):
    return (value + step - 1) // step * step


def sort_pairs(count):
    pairs = []
    p = 1
    while p < count:
        k = p
        while k >= 1:
            for j in range(k % p, count - k, 2 * k):
                for i in range(min(k, count - j - k)):
                    if (i + j) // (2 * p) == (i + j + k) // (2 * p):
                        pairs.append((i + j, i + j + k))
            k //= 2
        p *= 2
    return pairs


def steps(pair):
    return bin(pair).count("1")


class Packing:
    def __init__(self, units, lon):
        self.units, self.full, self.tail = units, lon // LANES, lon % LANES
        self.beside = LANES // self.tail if self.tail else 1
        self.tails = round_up(units, self.beside) // self.beside if self.tail else 0
        self.lines = units * self.full + self.tails
        self.used = (units - 1) % self.beside * self.tail + self.tail

    def line(self, load, number):
        if number >= self.tails:
            number -= self.tails
            return load(number // self.full, number % self.full * LANES, LANES)
        first = number * self.beside
        last = min(first + self.beside, self.units)
        parts = [load(u, self.full * LANES, self.tail) for u in range(first, last)]
        empty = LANES - self.tail * len(parts)
        if empty:
            parts.append(jnp.zeros((SUBLANES, empty), jnp.float32))
        return jnp.concatenate(parts, axis=1) if len(parts) > 1 else parts[0]

    def mask(self, unit, line, lane):
        start = self.tails + unit * self.full
        inside = (line >= start) & (line < start + self.full)
        if self.tail:
            low = unit % self.beside * self.tail
            inside |= (line == unit // self.beside) & (lane >= low) & (lane < low + self.tail)
        return inside

    def pieces(self):
        for u in range(self.units):
            for c in range(self.full):
                yield u, c * LANES, LANES, self.tails + u * self.full + c, 0
            if self.tail:
                yield u, self.full * LANES, self.tail, u // self.beside, u % self.beside * self.tail


class Layout:
    def __init__(self, held, lines):
        whole = lines // SUBLANES * SUBLANES
        cuts = [0, whole - SUBLANES, whole, lines]
        self.held, self.whole, self.moved = held, whole, lines - whole
        self.pitch = round_up(held * lines, SUBLANES)
        self.chunks = [(held * low, held * (high - low)) for low, high in zip(cuts, cuts[1:])]
        self.lines = [(low, high - low) for low, high in zip(cuts, cuts[1:])]

    def row(self, m, line):
        for low, size in self.lines:
            if line < low + size:
                return self.held * low + m * size + line - low


def kernel(
    n, nz, ens_ref, obs_ref, mask_ref, band_ref, field_ref, table_ref,
    ens_v, obs_v, mask_s, packet, obs_rows, gathered, ends, sums, back, partials,
    load_sem, send_sem, recv_sem, share_sem, round_sem, wave_sem,
):
    held, variables, leads, rows, lon = ens_ref.shape
    units = variables * leads
    packing = Packing(units, lon)
    lines = packing.lines
    layout = Layout(held, lines)
    pitch, whole, moved = layout.pitch, layout.whole, layout.moved
    stride = obs_rows.shape[0] // n
    slots = n * held
    total = n * nz
    chips = n // 2
    depth = max(steps(pair) for pair in range(chips))
    bits = [1 << b for b in range(depth)]
    me = lax.axis_index("member")
    band = lax.axis_index("lat")
    mine = band * n + me
    flag_line = packing.tails - 1

    rest, change, held_bit = me, {}, {}
    for bit in [2 * bit for bit in bits[::-1]] + [1]:
        held_bit[bit] = rest >= bit
        change[bit] = jnp.where(held_bit[bit], -bit, bit)
        rest = jnp.where(held_bit[bit], rest - bit, rest)
    first_core = me - jnp.where(held_bit[1], 1, 0)

    def beside(pair, c):
        return first_core + sum(change[2 * bit] for bit in bits if pair & bit) + c

    partner = me + change[1]
    near = [beside(bit, c) for c in range(2) for bit in bits] + [partner]
    above = {"member": me, "lat": lax.rem(band + 1, nz)}
    below = {"member": me, "lat": lax.rem(band + nz - 1, nz)}
    has_above = band < nz - 1
    has_below = band > 0

    def signal(sem, peer):
        pl.semaphore_signal(sem, inc=1, device_id=peer, device_id_type=MESH)

    mask_load = pltpu.make_async_copy(mask_ref, mask_s, load_sem.at[held + 1])
    ens_loads = [pltpu.make_async_copy(ens_ref.at[m], ens_v.at[m], load_sem.at[m]) for m in range(held)]
    obs_load = pltpu.make_async_copy(obs_ref, obs_v, load_sem.at[held])
    for load in [obs_load, mask_load] + ens_loads:
        load.start()
    barrier = pltpu.get_barrier_semaphore()
    for to in near:
        signal(barrier, {"member": to, "lat": band})
    pl.when(has_above)(lambda: signal(barrier, above))
    pl.when(has_below)(lambda: signal(barrier, below))

    mask_load.wait()
    obs_load.wait()
    free = lax.broadcasted_iota(jnp.int32, (SUBLANES, LANES), 1) >= packing.used

    def obs_line(block, line):
        def load(u, low, wide):
            return obs_v[u // leads, u % leads, pl.ds(block, SUBLANES), pl.ds(low, wide)]

        return packing.line(load, line)

    def pack(m, which):
        flag = jnp.full((SUBLANES, LANES), mask_s[m], jnp.int32)
        keep = flag != 0
        for block in range(0, rows, SUBLANES):

            def load(u, low, wide):
                return ens_v[m, u // leads, u % leads, pl.ds(block, SUBLANES), pl.ds(low, wide)]

            for line in which:
                value = jnp.where(keep, packing.line(load, line), obs_line(block, line))
                if line == flag_line:
                    value = jnp.where(free, flag.astype(jnp.float32), value)
                at = block * pitch + layout.row(m, line)
                packet[pl.ds(at, SUBLANES, stride=pitch), :] = value

    def send(chunk, to):
        low, size = layout.chunks[chunk]
        pltpu.make_async_remote_copy(
            src_ref=packet.at[pl.ds(pl.multiple_of(to * pitch + low, SUBLANES), size)],
            dst_ref=gathered.at[pl.ds(pl.multiple_of(me * pitch + low, SUBLANES), size)],
            send_sem=send_sem,
            recv_sem=recv_sem.at[chunk],
            device_id={"member": to, "lat": band},
            device_id_type=MESH,
        ).start()

    def send_ends(to):
        low, size = layout.chunks[2]
        for which in range(2):
            pltpu.make_async_remote_copy(
                src_ref=packet.at[pl.ds(pl.multiple_of((to + 2 * which) * pitch + low, SUBLANES), size)],
                dst_ref=ends.at[pl.ds(pl.multiple_of((2 * me + which) * SUBLANES, SUBLANES), size)],
                send_sem=send_sem,
                recv_sem=recv_sem.at[1],
                device_id={"member": to, "lat": band},
                device_id_type=MESH,
            ).start()

    def send_rows(pairs, cores, parts=(0, 1)):
        for c in cores:
            for pair in pairs:
                to = beside(pair, c)
                for part in parts:
                    send(part, to)
                if 1 in parts:
                    pl.when(held_bit[2] if pair % 2 else helps)(lambda: send_ends(to))

    helps = jnp.logical_not(held_bit[2])

    across, along = bits[: (depth + 1) // 2], bits[(depth + 1) // 2 :]

    for m in range(held):
        ens_loads[m].wait()
        pack(m, range(lines))
    count_near = len(near) + (band + nz - 1) // nz + (2 * nz - 2 - band) // nz
    pl.semaphore_wait(barrier, count_near)
    def tell(far):
        for bit in bits:
            peer = me + change[2 * bit]
            low_kept = jnp.logical_not(held_bit[2]) if bit == 1 else held_bit[2] | (peer < 2)
            low_kept = low_kept | (peer < 2) if bit == 1 else low_kept
            go = functools.partial(signal, round_sem.at[far - 2], {"member": peer, "lat": band})
            if bit == bits[0]:
                pl.when(low_kept)(go)
            elif bit == bits[-1]:
                pl.when(jnp.logical_not(low_kept))(go)
            else:
                go()

    tell(2)
    toward = held_bit[2]
    straight = held_bit[4]
    send_rows(across, [0])
    send_rows(along, [0])
    pl.when((me < 2) | (straight & toward))(lambda: send_rows(across, [1], [0]))
    pl.when(straight & toward)(lambda: send_rows(across, [1], [1]))
    send_rows(along, [1])
    for far in range(2, depth + 1):
        if far > 2:
            tell(far)
        else:
            send(0, partner)
            send(1, partner)
            pl.when(helps)(lambda: send_ends(partner))
        pl.semaphore_wait(round_sem.at[far - 2], depth - 1)
        diagonal = [pair for pair in range(chips) if steps(pair) == far]
        send_rows(diagonal, [0])
        if far == 2:
            pl.when(straight & jnp.logical_not(toward))(lambda: send_rows(across, [1], [0]))
        send_rows(diagonal, [1])
    pl.when(toward & jnp.logical_not(straight))(lambda: send_rows(across, [1], [0]))
    pl.when(jnp.logical_not(straight & toward))(lambda: send_rows(across, [1], [1]))
    pl.when(band == nz - 1)(lambda: signal(wave_sem.at[1], below))
    for block in range(0, rows, SUBLANES):
        for line in range(lines):
            obs_rows[pl.ds(block * stride + line, SUBLANES, stride=stride), :] = obs_line(block, line)
    own = pl.ds(pl.multiple_of(me * pitch, SUBLANES), pitch)
    gathered[own, :] = packet[own, :]

    @pl.when(helps)
    def _():
        low, size = layout.chunks[2]
        for which in range(2):
            mine_at = pl.ds(pl.multiple_of((2 * me + which) * SUBLANES, SUBLANES), size)
            ends[mine_at, :] = packet[pl.ds(pl.multiple_of((me + 2 * which) * pitch + low, SUBLANES), size), :]

    pl.when(has_below)(lambda: pl.semaphore_wait(wave_sem.at[0], 1))
    pl.when(has_above)(lambda: signal(wave_sem.at[0], above))

    def weight_of(row):
        number = jnp.full((1, LANES), band_ref[0] + row, jnp.int32).astype(jnp.float32)
        return jnp.cos((90.0 - number * 180.0 / (GRID_LAT - 1)) * math.pi / 180.0)

    weight, other_weight = weight_of(me), weight_of(me + 2)
    pl.when(has_above)(lambda: pl.semaphore_wait(wave_sem.at[1], 1))
    pl.when(has_above & has_below)(lambda: signal(wave_sem.at[1], below))

    def arrived(sem, ref, size):
        whole = ref.at[pl.ds(0, size)]
        pltpu.make_async_copy(whole, whole, sem).wait()

    network = sort_pairs(slots)
    lane = lax.broadcasted_iota(jnp.int32, (SUBLANES, LANES), 1)
    below_line = lax.broadcasted_iota(jnp.int32, (SUBLANES, LANES), 0)
    raw = []

    def crps(x, truth):
        x = list(x)
        skill = functools.reduce(jnp.add, [jnp.abs(value - truth) for value in x])
        for a, b in network:
            x[a], x[b] = jnp.minimum(x[a], x[b]), jnp.maximum(x[a], x[b])
        spread = functools.reduce(
            jnp.add,
            [(slots - 1.0 - 2.0 * i) * (x[slots - 1 - i] - x[i]) for i in range(slots // 2)],
        )
        return (slots - 1.0) * skill - spread

    def by_unit(score, line):
        return [jnp.where(packing.mask(u, line, lane), score, 0.0) for u in range(units)]

    def put(score, j, size):
        for u, low, wide, at, first in packing.pieces():
            if j <= at < j + size:
                field_ref[u // leads, u % leads, :, pl.ds(low, wide)] = score[at - j : at - j + 1, first : first + wide]

    arrived(recv_sem.at[0], gathered, (n - 1) * layout.chunks[0][1])
    parts = None
    for j in range(0, whole, SUBLANES):
        if j == layout.lines[1][0]:
            late, end = (n - 1) * layout.chunks[1][1], 2 * (n - 1) * layout.chunks[2][1]
            pl.when(helps)(lambda: arrived(recv_sem.at[1], gathered, late + end))
            pl.when(held_bit[2])(lambda: arrived(recv_sem.at[1], gathered, late))
        x = [
            gathered[pl.ds(s // held * pitch + layout.row(s % held, j), SUBLANES), :]
            for s in range(slots)
        ]
        if j == 0:
            flags = functools.reduce(jnp.add, x)
            flags = jnp.where((below_line == flag_line) & free, flags, 0.0)
            count = jnp.max(jnp.max(flags, axis=0, keepdims=True), axis=1, keepdims=True)
            scale = 1.0 / (count * (count - 1.0))
        raw.append(crps(x, obs_rows[pl.ds(pl.multiple_of(me * stride + j, SUBLANES), SUBLANES), :]))
        more = by_unit(raw[-1], below_line + j)
        parts = more if parts is None else [a + b for a, b in zip(parts, more)]
    for u in range(units):
        sums[u] = parts[u] * weight

    @pl.when(helps)
    def _():
        upper = below_line < moved
        x = []
        for s in range(slots):
            at = s // held * 2 * SUBLANES + s % held * moved
            mine_here = ends[pl.ds(at, SUBLANES), :]
            x.append(jnp.where(upper, mine_here, ends[pl.ds(at + SUBLANES - moved, SUBLANES), :]))
        truth = jnp.where(
            upper,
            obs_rows[pl.ds(me * stride + whole, SUBLANES), :],
            obs_rows[pl.ds((me + 2) * stride + whole - moved, SUBLANES), :],
        )
        score = crps(x, truth)
        back[pl.ds(0, SUBLANES), :] = score
        weighed = jnp.where(below_line < 2 * moved, score, 0.0) * jnp.where(upper, weight, other_weight)
        line = jnp.where(upper, below_line, below_line - moved) + whole
        for u, part in enumerate(by_unit(weighed, line)):
            sums[u] += part

    lane = lax.broadcasted_iota(jnp.int32, (1, LANES), 1)
    row = jnp.zeros((1, LANES), jnp.float32)
    for u in range(units):
        one = jnp.sum(jnp.sum(sums[u], axis=0, keepdims=True), axis=1, keepdims=True)
        row = jnp.where(lane == u, one, row)
    partials[pl.ds(mine, 1), :] = row * scale

    def share_with(far):
        return pltpu.make_async_remote_copy(
            src_ref=partials.at[pl.ds(mine, 1)],
            dst_ref=partials.at[pl.ds(mine, 1)],
            send_sem=send_sem,
            recv_sem=share_sem,
            device_id={"member": far % n, "lat": far // n},
            device_id_type=MESH,
        )

    for far in range(total):
        pl.when(far != mine)(lambda far=far: share_with(far).start())
    give_back = pltpu.make_async_remote_copy(
        src_ref=back.at[pl.ds(0, SUBLANES)],
        dst_ref=back.at[pl.ds(SUBLANES, SUBLANES)],
        send_sem=send_sem,
        recv_sem=share_sem,
        device_id={"member": me + change[2], "lat": band},
        device_id_type=MESH,
    )
    pl.when(helps)(lambda: give_back.start())
    for j, score in enumerate(raw):
        put(score * scale, j * SUBLANES, SUBLANES)
    sent = (n - 1) * held * whole + total - 1

    @pl.when(helps)
    def _():
        put(back[pl.ds(0, SUBLANES), :] * scale, whole, moved)
        arrived(send_sem, packet, sent + (n - 2) * layout.chunks[2][1] + SUBLANES)
        arrived(share_sem, packet, total - 1)

    @pl.when(held_bit[2])
    def _():
        arrived(send_sem, packet, sent + n * layout.chunks[2][1])
        arrived(share_sem, packet, total - 1 + SUBLANES)
        put(back[pl.ds(SUBLANES + moved, SUBLANES), :] * scale, whole, moved)

    summed = jnp.sum(partials[...], axis=0, keepdims=True)
    table_ref[...] = summed[:, :units] / (nz * rows * lon)


def write_out(field_ref, table_ref, field_out, table_out, sem):
    copies = [
        pltpu.make_async_copy(field_ref, field_out, sem.at[0]),
        pltpu.make_async_copy(table_ref, table_out, sem.at[1]),
    ]
    for copy in copies:
        copy.start()
    for copy in copies:
        copy.wait()


def on_device(n, nz, ensemble, observation, valid_mask, band_start):
    held, variables, leads, rows, lon = ensemble.shape
    assert rows == n and rows % SUBLANES == 0
    units = variables * leads
    packing = Packing(units, lon)
    assert packing.tails and packing.used < LANES
    layout = Layout(held, packing.lines)
    assert packing.lines >= 2 * SUBLANES and 0 < layout.moved <= SUBLANES // 2
    assert held * layout.moved <= SUBLANES and held * layout.whole % SUBLANES == 0
    pitch = layout.pitch
    depth = max(steps(pair) for pair in range(n // 2))
    assert depth > 1 and n == 2 ** (depth + 1)
    stride = round_up(packing.lines + SUBLANES, SUBLANES)
    total = n * nz
    field, table = pl.pallas_call(
        functools.partial(kernel, n, nz),
        out_shape=(
            pltpu.VMEM((variables, leads, rows // n, lon), jnp.float32),
            pltpu.VMEM((1, units), jnp.float32),
        ),
        in_specs=[pl.BlockSpec(memory_space=pltpu.HBM)] * 3 + [pl.BlockSpec(memory_space=pltpu.SMEM)],
        out_specs=(
            pl.BlockSpec(memory_space=pltpu.VMEM),
            pl.BlockSpec(memory_space=pltpu.VMEM),
        ),
        scratch_shapes=[
            pltpu.VMEM(ensemble.shape, jnp.float32),
            pltpu.VMEM(observation.shape, jnp.float32),
            pltpu.SMEM(valid_mask.shape, jnp.int32),
            pltpu.VMEM((n * pitch, LANES), jnp.float32),
            pltpu.VMEM((n * stride, LANES), jnp.float32),
            pltpu.VMEM((n * pitch + SUBLANES, LANES), jnp.float32),
            pltpu.VMEM((2 * n * SUBLANES + SUBLANES, LANES), jnp.float32),
            pltpu.VMEM((units, SUBLANES, LANES), jnp.float32),
            pltpu.VMEM((3 * SUBLANES, LANES), jnp.float32),
            pltpu.VMEM((total, LANES), jnp.float32),
            pltpu.SemaphoreType.DMA((held + 2,)),
            pltpu.SemaphoreType.DMA,
            pltpu.SemaphoreType.DMA((2,)),
            pltpu.SemaphoreType.DMA,
            pltpu.SemaphoreType.REGULAR((depth - 1,)),
            pltpu.SemaphoreType.REGULAR((2,)),
        ],
        compiler_params=pltpu.CompilerParams(
            collective_id=0, has_side_effects=True, vmem_limit_bytes=VMEM_BYTES
        ),
        name="fair_crps",
    )(ensemble, observation, valid_mask, band_start)
    field, table = pl.pallas_call(
        write_out,
        out_shape=(
            jax.ShapeDtypeStruct(field.shape, jnp.float32),
            jax.ShapeDtypeStruct(table.shape, jnp.float32),
        ),
        in_specs=[pl.BlockSpec(memory_space=pltpu.VMEM)] * 2,
        out_specs=(pl.BlockSpec(memory_space=pltpu.HBM),) * 2,
        scratch_shapes=[pltpu.SemaphoreType.DMA((2,))],
        name="write_out",
    )(*(pltpu.with_memory_space_constraint(a, pltpu.VMEM) for a in (field, table)))
    return field, table.reshape(variables, leads)


def solution(mesh):
    placed = (
        P("member", None, None, "lat", None),
        P(None, None, "lat", None),
        P("member"),
        P("lat"),
    )
    return jax.shard_map(
        functools.partial(on_device, mesh.shape["member"], mesh.shape["lat"]),
        mesh=mesh,
        in_specs=placed,
        out_specs=(P(None, None, ("lat", "member"), None), P()),
        check_vma=False,
    )
```
